32 devices in a mesh: cells: 8 (over z, x), views: 4 (over y, core).
Axes of the slice: x: 2, y: 2, z: 4, core: 2. Of those that a mesh axis runs over, the one named last changes fastest.
Arguments:
- params: float32 [59, 16384], P(None, 'cells'), may hold values from -5 to 4, as said below
- first_moment: float32 [59, 16384], P(None, 'cells'), may hold values from -0.6 to 0.6
- second_moment: float32 [59, 16384], P(None, 'cells'), may hold values from 1e-12 to 0.05
- cameras: float32 [4, 6], P('views'), may hold values from -0.004 to 0.004
- visible: int32 [4, 16384], P('views', 'cells'), may hold values from 0 to 1, as said below
- send_plan: int32 [4, 8, 8, 256], P('views', 'cells'), may hold values from -1 to 2047, as said below
- tile_lists: int32 [4, 32, 512], P('views', 'cells'), may hold values from -1 to 2047, as said below
- target: float32 [4, 3, 8192], P('views', None, 'cells'), may hold values from 0 to 1
Outputs:
- updated_params: float32 [59, 16384], P(None, 'cells')
- updated_first: float32 [59, 16384], P(None, 'cells')
- updated_second: float32 [59, 16384], P(None, 'cells')
The draws below stay inside these ranges and needn't reach their ends.
Inputs may be any that keep to these rules, and one draw needn't show every extreme that they name: `params`: rows 0 to 2 hold a Gaussian's mean, 3 to 5 the logarithms of its scales, 6 to 9 a rotation quaternion whose first component is at least 0.6, 10 its opacity logit, 11 to 58 its spherical-harmonic coefficients; every Gaussian lies at depth 2 or more before every camera. In each view, between a quarter and three quarters of each owner's block of 2048 Gaussians are visible. Every row of an owner's block of 2048 Gaussians belongs to exactly one rendering device, 256 rows to each device; send_plan[v, s, d, :] lists exactly the rows of owner s that belong to device d and are visible in view v, live entries first, then -1; in every view some device receives 256 rows from every owner. `tile_lists`: tile t is rendered on device t // 4; an entry e stands for send_plan[v, e // 256, t // 4, e % 256], which is live; live entries come first, ordered by increasing params[2] of their Gaussians, then -1; some tile of each view has 512 live entries.
All inputs are finite; a program needn't handle non-finite values.
Results may differ from the reference program's by a relative error of at most 0.0003.
Values sent between devices are 32-bit elements; how exact they have to be, the bound alone decides.
A program may use at most 64 MiB of HBM per device.

```python
import jax
import jax.numpy as jnp
from jax import lax

G_DEV = 2048
TILES_DEV = 4
L = 512
TILE_COLS = 32
ADAM_STEP = 1000
CAP = 256
VIEWS = 4
OWNERS = 8
GAUSSIANS = 16384
TILES = 32
N_CELLS = 8
N_VIEWS = 4


def draw_scene(key):
    block_cols = TILE_COLS // 4
    block_high = 4 * TILES_DEV
    hot_rows = (L + OWNERS - 1) // OWNERS
    widest = min(27, (block_high - 1) // 2)
    reach_span = widest - 5
    shape_rows = (OWNERS, G_DEV)
    local_ids = jnp.arange(G_DEV, dtype=jnp.int32)
    placement = jnp.argsort(jax.random.randint(jax.random.fold_in(key, 301), shape_rows, 0, 4096) * G_DEV + local_ids[None, :], axis=-1).astype(jnp.int32)
    home_owner = placement // CAP
    within = placement % CAP
    edge_splat = (within == CAP - 1) & (within >= hot_rows) & (home_owner < block_cols)
    hot_tile = jax.random.randint(jax.random.fold_in(key, 302), (OWNERS,), 0, TILES_DEV)
    random_tile = jax.random.randint(jax.random.fold_in(key, 303), shape_rows, 0, TILES_DEV)
    aim_tile = jnp.where(within < hot_rows, hot_tile[home_owner], random_tile)
    aim_across = 16 * (aim_tile % 4) + jax.random.randint(jax.random.fold_in(key, 304), shape_rows, 0, 16)
    aim_down = 16 * (aim_tile // 4) + jax.random.randint(jax.random.fold_in(key, 305), shape_rows, 0, 16)
    reach = 6 + jnp.minimum(jax.random.randint(jax.random.fold_in(key, 306), shape_rows, 0, reach_span), jax.random.randint(jax.random.fold_in(key, 307), shape_rows, 0, reach_span))
    centre_across = jnp.clip(aim_across, reach, 63 - reach)
    centre_down = jnp.clip(aim_down, reach, block_high - 1 - reach)
    first_col = jnp.where(edge_splat, (aim_across - 28) // 16, (centre_across - reach) // 16)
    last_col = jnp.where(edge_splat, (aim_across + 28) // 16, (centre_across + reach) // 16)
    first_row = jnp.where(edge_splat, 0, (centre_down - reach) // 16)
    last_row = jnp.where(edge_splat, 0, (centre_down + reach) // 16)
    pixel_across = 64 * (home_owner % block_cols) + jnp.where(edge_splat, aim_across, centre_across)
    pixel_down = jnp.where(edge_splat, -48, block_high * (home_owner // block_cols) + centre_down)
    depth_keys = jax.random.randint(jax.random.fold_in(key, 308), (GAUSSIANS,), 0, 1024) * GAUSSIANS + jnp.arange(GAUSSIANS, dtype=jnp.int32)
    depth_rank = jnp.argsort(depth_keys).astype(jnp.int32).reshape(OWNERS, G_DEV)
    front_owner = jax.random.randint(jax.random.fold_in(key, 309), (VIEWS, 1, 1), 0, OWNERS)
    drawn = jax.random.randint(jax.random.fold_in(key, 310), (VIEWS, OWNERS, 1), G_DEV // 4, 3 * G_DEV // 4 + 1)
    noise = jax.random.randint(jax.random.fold_in(key, 311), (VIEWS, OWNERS, G_DEV), 0, 1024)
    scores = jnp.where(home_owner[None] == front_owner, 0, 1024 * G_DEV) + noise * G_DEV + local_ids[None, None, :]
    ranks = jnp.argsort(jnp.argsort(scores, axis=-1), axis=-1)
    seen = ranks < drawn
    visible = seen.astype(jnp.int32).reshape(VIEWS, GAUSSIANS)
    home_rows = jnp.argsort(placement, axis=-1).astype(jnp.int32)
    seen_home = jnp.take_along_axis(seen, jnp.broadcast_to(home_rows[None], (VIEWS, OWNERS, G_DEV)), axis=2).reshape(VIEWS, OWNERS, OWNERS, CAP)
    rows_home = jnp.broadcast_to(home_rows.reshape(1, OWNERS, OWNERS, CAP), (VIEWS, OWNERS, OWNERS, CAP))
    slot_ids = jnp.arange(CAP, dtype=jnp.int32)
    compact = jnp.argsort(jnp.where(seen_home, slot_ids, CAP + slot_ids), axis=-1)
    plan = jnp.where(jnp.take_along_axis(seen_home, compact, axis=3), jnp.take_along_axis(rows_home, compact, axis=3), -1).astype(jnp.int32)
    safe_rows = jnp.maximum(plan, 0)
    sources = jnp.arange(OWNERS, dtype=jnp.int32)[None, :, None, None]

    def per_slot(table):
        return jnp.transpose(table[sources, safe_rows], (0, 2, 1, 3)).reshape(VIEWS, OWNERS, 1, OWNERS * CAP)
    live = jnp.transpose(plan >= 0, (0, 2, 1, 3)).reshape(VIEWS, OWNERS, 1, OWNERS * CAP)
    tile_local = jnp.arange(TILES_DEV, dtype=jnp.int32)[None, None, :, None]
    tile_across = tile_local % 4
    tile_down = tile_local // 4
    meets = live & (per_slot(first_col) <= tile_across) & (per_slot(last_col) >= tile_across) & (per_slot(first_row) <= tile_down) & (per_slot(last_row) >= tile_down)
    slot_all = jnp.arange(OWNERS * CAP, dtype=jnp.int32)
    edge_ints = edge_splat.astype(jnp.int32)
    sort_key = jnp.where(meets, per_slot(depth_rank) + GAUSSIANS * (1 - per_slot(edge_ints)), 2 * GAUSSIANS + slot_all)
    order = jnp.argsort(sort_key, axis=-1)[..., :L].astype(jnp.int32)
    best = jnp.take_along_axis(sort_key, order, axis=-1)
    lists = jnp.where(best < 2 * GAUSSIANS, order, -1).astype(jnp.int32).reshape(VIEWS, OWNERS * TILES_DEV, L)
    return (visible, plan, lists, pixel_across, pixel_down, reach, depth_rank, edge_ints)


def draw_visible(key, part):
    return draw_scene(key)[0]


def draw_send_plan(key, part):
    return draw_scene(key)[1]


def draw_tile_lists(key, part):
    return draw_scene(key)[2]


def draw_params(key, part):
    scene = draw_scene(key)
    half_width = TILE_COLS * 8.0
    rows_pix = TILES // TILE_COLS * 16
    edge_splat = scene[7].reshape(GAUSSIANS) > 0
    rank_part = (scene[6].reshape(GAUSSIANS).astype(jnp.float32) + 0.5) / GAUSSIANS
    across = (scene[3].reshape(GAUSSIANS).astype(jnp.float32) + 0.5 - half_width) / half_width
    down = (scene[4].reshape(GAUSSIANS).astype(jnp.float32) + 0.5 - rows_pix * 0.5) / half_width
    depth = jnp.where(edge_splat, 2.05 + 0.4 * rank_part, 2.5 + 1.5 * rank_part)
    sigma_pix = (scene[5].reshape(GAUSSIANS).astype(jnp.float32) - 3.0) / 3.0
    jitter = jax.random.uniform(jax.random.fold_in(key, 201), (3, GAUSSIANS), jnp.float32, -0.15, 0.15)
    drawn_scale = jnp.log(sigma_pix * depth / half_width)[None, :] + jitter
    edge_scale = jnp.log(48.0 / half_width * depth / (5.4 * jnp.sqrt(1.0 + down * down)))
    log_scale = jnp.where(edge_splat[None, :], jnp.broadcast_to(edge_scale[None, :], (3, GAUSSIANS)), drawn_scale)
    quat_first = jax.random.uniform(jax.random.fold_in(key, 204), (1, GAUSSIANS), jnp.float32, 0.6, 1.2)
    quat_rest = jax.random.uniform(jax.random.fold_in(key, 205), (3, GAUSSIANS), jnp.float32, -1.0, 1.0)
    logit = jax.random.uniform(jax.random.fold_in(key, 206), (1, GAUSSIANS), jnp.float32, -3.5, -1.0)
    constant_part = jax.random.uniform(jax.random.fold_in(key, 207), (3, GAUSSIANS), jnp.float32, -1.5, 1.5)
    higher = jnp.clip(0.3 * jax.random.normal(jax.random.fold_in(key, 208), (45, GAUSSIANS), jnp.float32), -1.5, 1.5)
    edge_logit = jax.random.uniform(jax.random.fold_in(key, 211), (1, GAUSSIANS), jnp.float32, -1.5, -1.0)
    logit = jnp.where(edge_splat[None, :], edge_logit, logit)
    means = jnp.stack([across * depth, down * depth, depth])
    return jnp.concatenate([means, log_scale, quat_first, quat_rest, logit, constant_part, higher], axis=0)


def draw_moments(key):
    edge_splat = draw_scene(key)[7].reshape(GAUSSIANS) > 0
    faint_second = jnp.exp(jax.random.uniform(jax.random.fold_in(key, 402), (59, GAUSSIANS), jnp.float32, -27.631021, -25.328436))
    drawn_second = jnp.exp(jax.random.uniform(jax.random.fold_in(key, 403), (59, GAUSSIANS), jnp.float32, -6.9077553, -2.9957323))
    second = jnp.where(edge_splat[None, :], faint_second, drawn_second)
    drawn_first = jnp.clip(0.1 * jax.random.normal(jax.random.fold_in(key, 404), (59, GAUSSIANS), jnp.float32), -0.6, 0.6)
    faint_first = 0.3 * jnp.sqrt(faint_second) * jnp.clip(jax.random.normal(jax.random.fold_in(key, 405), (59, GAUSSIANS), jnp.float32), -2.0, 2.0)
    first = jnp.where(edge_splat[None, :], faint_first, drawn_first)
    return (first, second)


def draw_first_moment(key, part):
    return draw_moments(key)[0]


def draw_second_moment(key, part):
    return draw_moments(key)[1]


def levels(stream_key, extent, cuts, least, largest):
    level = 1.0
    for position, blocks in cuts:
        draws = jax.random.uniform(jax.random.fold_in(jax.random.fold_in(stream_key, 6), position), (blocks,), jnp.float32, least / len(cuts), largest / len(cuts))
        level = level * jnp.repeat(jnp.exp(draws), extent[position] // blocks).reshape((-1,) + (1,) * (len(extent) - 1 - position))
    return level


def setup_inputs(seed: int = 0) -> dict:
    keys = jax.random.split(jax.random.key(seed), 9)
    params = draw_params(jax.random.fold_in(keys[8], 71), 0)
    first_moment = draw_first_moment(jax.random.fold_in(keys[8], 71), 0)
    second_moment = draw_second_moment(jax.random.fold_in(keys[8], 71), 0)
    cameras = jnp.clip(jax.random.uniform(keys[3], (VIEWS, 6), jnp.float32, -0.004, 0.004) * levels(keys[3], (VIEWS, 6), ((0, 4),), -0.4, 0.0), -0.004, 0.004)
    visible = draw_visible(jax.random.fold_in(keys[8], 71), 0)
    send_plan = draw_send_plan(jax.random.fold_in(keys[8], 71), 0)
    tile_lists = draw_tile_lists(jax.random.fold_in(keys[8], 71), 0)
    target = jnp.clip(1.0 * jax.random.uniform(keys[7], (VIEWS, 3, TILES * 256), jnp.float32) ** levels(keys[7], (VIEWS, 3, TILES * 256), ((0, 4), (2, 8)), -0.2, 0.2), 0.0, 1.0)
    return {"params": params, "first_moment": first_moment, "second_moment": second_moment, "cameras": cameras, "visible": visible, "send_plan": send_plan, "tile_lists": tile_lists, "target": target}


harmonic_zero = 0.28209479177387814
harmonic_one = 0.4886025119029199
harmonic_two = (1.0925484305920792, -1.0925484305920792, 0.31539156525252005, -1.0925484305920792, 0.5462742152960396)
harmonic_three = (-0.5900435899266435, 2.890611442640554, -0.4570457994644658, 0.3731763325901154, -0.4570457994644658, 1.445305721320277, -0.5900435899266435)

def harmonics(across, upward, onward):
    across_sq = across * across
    upward_sq = upward * upward
    onward_sq = onward * onward
    return jnp.stack([harmonic_zero * jnp.ones_like(across), -harmonic_one * upward, harmonic_one * onward, -harmonic_one * across, harmonic_two[0] * across * upward, harmonic_two[1] * upward * onward, harmonic_two[2] * (2.0 * onward_sq - across_sq - upward_sq), harmonic_two[3] * across * onward, harmonic_two[4] * (across_sq - upward_sq), harmonic_three[0] * upward * (3.0 * across_sq - upward_sq), harmonic_three[1] * across * upward * onward, harmonic_three[2] * upward * (4.0 * onward_sq - across_sq - upward_sq), harmonic_three[3] * onward * (2.0 * onward_sq - 3.0 * across_sq - 3.0 * upward_sq), harmonic_three[4] * across * (4.0 * onward_sq - across_sq - upward_sq), harmonic_three[5] * onward * (across_sq - upward_sq), harmonic_three[6] * across * (across_sq - 3.0 * upward_sq)])

def camera_rotation(angles):
    cos_roll, sin_roll = (jnp.cos(angles[0]), jnp.sin(angles[0]))
    cos_pitch, sin_pitch = (jnp.cos(angles[1]), jnp.sin(angles[1]))
    cos_yaw, sin_yaw = (jnp.cos(angles[2]), jnp.sin(angles[2]))
    naught = jnp.zeros_like(cos_roll)
    unit_one = jnp.ones_like(cos_roll)
    roll = jnp.stack([jnp.stack([unit_one, naught, naught]), jnp.stack([naught, cos_roll, -sin_roll]), jnp.stack([naught, sin_roll, cos_roll])])
    pitch = jnp.stack([jnp.stack([cos_pitch, naught, sin_pitch]), jnp.stack([naught, unit_one, naught]), jnp.stack([-sin_pitch, naught, cos_pitch])])
    yawing = jnp.stack([jnp.stack([cos_yaw, -sin_yaw, naught]), jnp.stack([sin_yaw, cos_yaw, naught]), jnp.stack([naught, naught, unit_one])])
    inner_turn = jnp.dot(pitch, roll, precision=lax.Precision.HIGHEST)
    return jnp.dot(yawing, inner_turn, precision=lax.Precision.HIGHEST)

def project(values, camera):
    turn = camera_rotation(camera[0:3])
    offset = values[0:3] - camera[3:6][:, None]
    in_view = jnp.dot(turn, offset, precision=lax.Precision.HIGHEST)
    inv_depth = 1.0 / in_view[2]
    screen_col = in_view[0] * inv_depth
    screen_row = in_view[1] * inv_depth
    scales = jnp.exp(values[3:6])
    quat = values[6:10] / jnp.sqrt(lax.optimization_barrier(jnp.sum(values[6:10] * values[6:10], axis=0, keepdims=True)))
    quat_w, quat_x, quat_y, quat_z = (quat[0], quat[1], quat[2], quat[3])
    spin = [[1.0 - 2.0 * (quat_y * quat_y + quat_z * quat_z), 2.0 * (quat_x * quat_y - quat_w * quat_z), 2.0 * (quat_x * quat_z + quat_w * quat_y)], [2.0 * (quat_x * quat_y + quat_w * quat_z), 1.0 - 2.0 * (quat_x * quat_x + quat_z * quat_z), 2.0 * (quat_y * quat_z - quat_w * quat_x)], [2.0 * (quat_x * quat_z - quat_w * quat_y), 2.0 * (quat_y * quat_z + quat_w * quat_x), 1.0 - 2.0 * (quat_x * quat_x + quat_y * quat_y)]]
    basis_cam = []
    for outer_index in range(3):
        row_terms = []
        for col_index in range(3):
            entry = turn[outer_index, 0] * spin[0][col_index]
            for mid_index in range(1, 3):
                entry = entry + turn[outer_index, mid_index] * spin[mid_index][col_index]
            row_terms.append(entry * scales[col_index])
        basis_cam.append(row_terms)
    jac_top = [(basis_cam[0][col_index] - screen_col * basis_cam[2][col_index]) * inv_depth for col_index in range(3)]
    jac_low = [(basis_cam[1][col_index] - screen_row * basis_cam[2][col_index]) * inv_depth for col_index in range(3)]
    sigma_a = jac_top[0] * jac_top[0] + jac_top[1] * jac_top[1] + jac_top[2] * jac_top[2]
    sigma_b = jac_top[0] * jac_low[0] + jac_top[1] * jac_low[1] + jac_top[2] * jac_low[2]
    sigma_c = jac_low[0] * jac_low[0] + jac_low[1] * jac_low[1] + jac_low[2] * jac_low[2]
    determinant = sigma_a * sigma_c - sigma_b * sigma_b
    opacity = jax.nn.sigmoid(values[10])
    distance = jnp.sqrt(lax.optimization_barrier(jnp.sum(offset * offset, axis=0)))
    unit_dir = offset / distance
    basis = harmonics(unit_dir[0], unit_dir[1], unit_dir[2])
    coeffs = values[11:59].reshape(16, 3, values.shape[1])
    colors = 0.5 + lax.optimization_barrier(jnp.sum(basis[:, None, :] * coeffs, axis=0))
    screen = jnp.stack([screen_col, screen_row, sigma_c / determinant, -sigma_b / determinant, sigma_a / determinant, opacity])
    return jnp.concatenate([screen, colors], axis=0)

def group_loss(pieces):
    features, live_mask, pixel_column, pixel_row, target_tile = pieces
    entries = live_mask.shape[1]
    delta_col = pixel_column[:, :, None] - features[0][:, None, :]
    delta_row = pixel_row[:, :, None] - features[1][:, None, :]
    power = -0.5 * (features[2][:, None, :] * delta_col * delta_col + 2.0 * features[3][:, None, :] * delta_col * delta_row + features[4][:, None, :] * delta_row * delta_row)
    alphas = features[5][:, None, :] * jnp.exp(power) * live_mask[:, None, :]
    log_keep = jnp.log(1.0 - alphas)
    earlier = (lax.broadcasted_iota(jnp.int32, (entries, entries), 0) < lax.broadcasted_iota(jnp.int32, (entries, entries), 1)).astype(jnp.float32)
    transmit = jnp.exp(jnp.einsum('bpl,lm->bpm', log_keep, earlier, precision=lax.Precision.HIGHEST))
    weights = alphas * transmit
    image = jnp.einsum('bpl,kbl->kbp', weights, features[6:9], precision=lax.Precision.HIGHEST)
    error = image - target_tile
    return jnp.sum(error * error)

def render_tiles(picked, live_mask, pixel_column, pixel_row, target_tile):
    groups = live_mask.shape[0] // 4
    entries = live_mask.shape[1]
    pixels = pixel_column.shape[1]
    stacked = (jnp.transpose(picked.reshape(picked.shape[0], groups, 4, entries), (1, 0, 2, 3)), live_mask.reshape(groups, 4, entries), pixel_column.reshape(groups, 4, pixels), pixel_row.reshape(groups, 4, pixels), jnp.transpose(target_tile.reshape(3, groups, 4, pixels), (1, 0, 2, 3)))
    return jnp.sum(lax.map(jax.checkpoint(group_loss), stacked))

def pixel_grid(first_tile, count, tiles_dev, rows_pix):
    tile_ids = first_tile + jnp.arange(count, dtype=jnp.int32)
    pixel_ids = jnp.arange(256, dtype=jnp.int32)
    block_cols = TILE_COLS // 4
    owner_ids = tile_ids // tiles_dev
    local_ids = tile_ids % tiles_dev
    tile_col = 4 * (owner_ids % block_cols) + local_ids % 4
    tile_row = tiles_dev // 4 * (owner_ids // block_cols) + local_ids // 4
    half_width = TILE_COLS * 8.0
    column = (tile_col[:, None] * 16 + pixel_ids[None, :] % 16).astype(jnp.float32)
    row_pos = (tile_row[:, None] * 16 + pixel_ids[None, :] // 16).astype(jnp.float32)
    return ((column + 0.5 - half_width) / half_width, (row_pos + 0.5 - rows_pix * 0.5) / half_width)

def adam_update(params, first_moment, second_moment, gradient, counts):
    row_ids = lax.broadcasted_iota(jnp.int32, params.shape, 0)
    rates = jnp.where(row_ids < 6, 0.01, jnp.where(row_ids < 10, 0.005, jnp.where(row_ids < 11, 0.05, jnp.where(row_ids < 14, 0.0025, 0.000125))))
    first_new = 0.9 * first_moment + 0.1 * gradient
    second = 0.999 * second_moment + 0.001 * gradient * gradient
    bias_one = 1.0 - 0.9 ** ADAM_STEP
    bias_two = 1.0 - 0.999 ** ADAM_STEP
    stride = rates * (first_new / bias_one) / (jnp.sqrt(second / bias_two) + 1e-08)
    seen_mask = counts > 0.0
    return (jnp.where(seen_mask, params - stride, params), jnp.where(seen_mask, first_new, first_moment), jnp.where(seen_mask, second, second_moment))

def reference(params, first_moment, second_moment, cameras, visible, send_plan, tile_lists, target):
    tiles_all = tile_lists.shape[1]
    tiles_dev = tiles_all // N_CELLS
    capacity = send_plan.shape[3]
    block = params.shape[1] // N_CELLS
    rows_pix = tiles_all // TILE_COLS * 16
    pixel_column, pixel_row = pixel_grid(0, tiles_all, tiles_dev, rows_pix)
    device_of = (jnp.arange(tiles_all, dtype=jnp.int32) // tiles_dev)[:, None]

    def view_loss(values, view_index):
        features = project(values, cameras[view_index])
        lists = tile_lists[view_index]
        live_mask = (lists >= 0).astype(jnp.float32)
        slot_ids = jnp.maximum(lists, 0)
        source = slot_ids // capacity
        column = slot_ids % capacity
        local_row = send_plan[view_index][source, device_of, column]
        global_row = (source * block + jnp.maximum(local_row, 0)).astype(jnp.int32)
        picked = jnp.take(features, global_row, axis=1)
        target_tile = target[view_index].reshape(3, tiles_all, 256)
        return render_tiles(picked, live_mask, pixel_column, pixel_row, target_tile)

    def total_loss(values):
        total = jnp.zeros((), jnp.float32)
        for view_index in range(N_VIEWS):
            total = total + view_loss(values, view_index)
        return total
    gradient = jax.grad(total_loss)(params)
    counts = lax.optimization_barrier(jnp.sum(visible.astype(jnp.float32), axis=0, keepdims=True))
    new_params, new_first, new_second = adam_update(params, first_moment, second_moment, gradient, counts)
    return (new_params, new_first, new_second)
```

```python
import functools

import jax
import jax.numpy as jnp
from jax import lax
from jax.experimental import pallas as pl
from jax.experimental.pallas import tpu as pltpu
from jax.sharding import PartitionSpec as P

TILE_COLS = 32
ADAM_STEP = 1000


harmonic_zero = 0.28209479177387814
harmonic_one = 0.4886025119029199
harmonic_two = (
    1.0925484305920792,
    -1.0925484305920792,
    0.31539156525252005,
    -1.0925484305920792,
    0.5462742152960396,
)
harmonic_three = (
    -0.5900435899266435,
    2.890611442640554,
    -0.4570457994644658,
    0.3731763325901154,
    -0.4570457994644658,
    1.445305721320277,
    -0.5900435899266435,
)


def harmonics(across, upward, onward):
    across_sq = across * across
    upward_sq = upward * upward
    onward_sq = onward * onward
    return jnp.stack(
        [
            harmonic_zero * jnp.ones_like(across),
            -harmonic_one * upward,
            harmonic_one * onward,
            -harmonic_one * across,
            harmonic_two[0] * across * upward,
            harmonic_two[1] * upward * onward,
            harmonic_two[2] * (2.0 * onward_sq - across_sq - upward_sq),
            harmonic_two[3] * across * onward,
            harmonic_two[4] * (across_sq - upward_sq),
            harmonic_three[0] * upward * (3.0 * across_sq - upward_sq),
            harmonic_three[1] * across * upward * onward,
            harmonic_three[2] * upward * (4.0 * onward_sq - across_sq - upward_sq),
            harmonic_three[3] * onward * (2.0 * onward_sq - 3.0 * across_sq - 3.0 * upward_sq),
            harmonic_three[4] * across * (4.0 * onward_sq - across_sq - upward_sq),
            harmonic_three[5] * onward * (across_sq - upward_sq),
            harmonic_three[6] * across * (across_sq - 3.0 * upward_sq),
        ]
    )


def camera_rotation(angles):
    cos_roll, sin_roll = (jnp.cos(angles[0]), jnp.sin(angles[0]))
    cos_pitch, sin_pitch = (jnp.cos(angles[1]), jnp.sin(angles[1]))
    cos_yaw, sin_yaw = (jnp.cos(angles[2]), jnp.sin(angles[2]))
    naught = jnp.zeros_like(cos_roll)
    unit_one = jnp.ones_like(cos_roll)
    roll = jnp.stack(
        [
            jnp.stack([unit_one, naught, naught]),
            jnp.stack([naught, cos_roll, -sin_roll]),
            jnp.stack([naught, sin_roll, cos_roll]),
        ]
    )
    pitch = jnp.stack(
        [
            jnp.stack([cos_pitch, naught, sin_pitch]),
            jnp.stack([naught, unit_one, naught]),
            jnp.stack([-sin_pitch, naught, cos_pitch]),
        ]
    )
    yawing = jnp.stack(
        [
            jnp.stack([cos_yaw, -sin_yaw, naught]),
            jnp.stack([sin_yaw, cos_yaw, naught]),
            jnp.stack([naught, naught, unit_one]),
        ]
    )
    inner_turn = jnp.dot(pitch, roll, precision=lax.Precision.HIGHEST)
    return jnp.dot(yawing, inner_turn, precision=lax.Precision.HIGHEST)


def project(values, camera):
    turn = camera_rotation(camera[0:3])
    offset = values[0:3] - camera[3:6][:, None]
    in_view = jnp.dot(turn, offset, precision=lax.Precision.HIGHEST)
    inv_depth = 1.0 / in_view[2]
    screen_col = in_view[0] * inv_depth
    screen_row = in_view[1] * inv_depth
    scales = jnp.exp(values[3:6])
    quat = values[6:10] / jnp.sqrt(jnp.sum(values[6:10] * values[6:10], axis=0, keepdims=True))
    quat_w, quat_x, quat_y, quat_z = (quat[0], quat[1], quat[2], quat[3])
    spin = [
        [
            1.0 - 2.0 * (quat_y * quat_y + quat_z * quat_z),
            2.0 * (quat_x * quat_y - quat_w * quat_z),
            2.0 * (quat_x * quat_z + quat_w * quat_y),
        ],
        [
            2.0 * (quat_x * quat_y + quat_w * quat_z),
            1.0 - 2.0 * (quat_x * quat_x + quat_z * quat_z),
            2.0 * (quat_y * quat_z - quat_w * quat_x),
        ],
        [
            2.0 * (quat_x * quat_z - quat_w * quat_y),
            2.0 * (quat_y * quat_z + quat_w * quat_x),
            1.0 - 2.0 * (quat_x * quat_x + quat_y * quat_y),
        ],
    ]
    basis_cam = []
    for outer_index in range(3):
        row_terms = []
        for col_index in range(3):
            entry = turn[outer_index, 0] * spin[0][col_index]
            for mid_index in range(1, 3):
                entry = entry + turn[outer_index, mid_index] * spin[mid_index][col_index]
            row_terms.append(entry * scales[col_index])
        basis_cam.append(row_terms)
    jac_top = [
        (basis_cam[0][col_index] - screen_col * basis_cam[2][col_index]) * inv_depth
        for col_index in range(3)
    ]
    jac_low = [
        (basis_cam[1][col_index] - screen_row * basis_cam[2][col_index]) * inv_depth
        for col_index in range(3)
    ]
    sigma_a = jac_top[0] * jac_top[0] + jac_top[1] * jac_top[1] + jac_top[2] * jac_top[2]
    sigma_b = jac_top[0] * jac_low[0] + jac_top[1] * jac_low[1] + jac_top[2] * jac_low[2]
    sigma_c = jac_low[0] * jac_low[0] + jac_low[1] * jac_low[1] + jac_low[2] * jac_low[2]
    determinant = sigma_a * sigma_c - sigma_b * sigma_b
    opacity = jax.nn.sigmoid(values[10])
    distance = jnp.sqrt(jnp.sum(offset * offset, axis=0))
    unit_dir = offset / distance
    basis = harmonics(unit_dir[0], unit_dir[1], unit_dir[2])
    coeffs = values[11:59].reshape(16, 3, values.shape[1])
    colors = 0.5 + jnp.sum(basis[:, None, :] * coeffs, axis=0)
    screen = jnp.stack(
        [
            screen_col,
            screen_row,
            sigma_c / determinant,
            -sigma_b / determinant,
            sigma_a / determinant,
            opacity,
        ]
    )
    return jnp.concatenate([screen, colors], axis=0)


def group_loss(pieces):
    features, live_mask, pixel_column, pixel_row, target_tile = pieces
    entries = live_mask.shape[1]
    delta_col = pixel_column[:, :, None] - features[0][:, None, :]
    delta_row = pixel_row[:, :, None] - features[1][:, None, :]
    power = -0.5 * (
        features[2][:, None, :] * delta_col * delta_col
        + 2.0 * features[3][:, None, :] * delta_col * delta_row
        + features[4][:, None, :] * delta_row * delta_row
    )
    alphas = features[5][:, None, :] * jnp.exp(power) * live_mask[:, None, :]
    log_keep = jnp.log(1.0 - alphas)
    earlier = (
        lax.broadcasted_iota(jnp.int32, (entries, entries), 0)
        < lax.broadcasted_iota(jnp.int32, (entries, entries), 1)
    ).astype(jnp.float32)
    transmit = jnp.exp(
        jnp.einsum("bpl,lm->bpm", log_keep, earlier, precision=lax.Precision.HIGHEST)
    )
    weights = alphas * transmit
    image = jnp.einsum("bpl,kbl->kbp", weights, features[6:9], precision=lax.Precision.HIGHEST)
    error = image - target_tile
    return jnp.sum(error * error)


def render_tiles(picked, live_mask, pixel_column, pixel_row, target_tile):
    groups = live_mask.shape[0] // 4
    entries = live_mask.shape[1]
    pixels = pixel_column.shape[1]
    stacked = (
        jnp.transpose(picked.reshape(picked.shape[0], groups, 4, entries), (1, 0, 2, 3)),
        live_mask.reshape(groups, 4, entries),
        pixel_column.reshape(groups, 4, pixels),
        pixel_row.reshape(groups, 4, pixels),
        jnp.transpose(target_tile.reshape(3, groups, 4, pixels), (1, 0, 2, 3)),
    )
    return jnp.sum(lax.map(jax.checkpoint(group_loss), stacked))


def pixel_grid(first_tile, count, tiles_dev, rows_pix):
    tile_ids = first_tile + jnp.arange(count, dtype=jnp.int32)
    pixel_ids = jnp.arange(256, dtype=jnp.int32)
    block_cols = TILE_COLS // 4
    owner_ids = tile_ids // tiles_dev
    local_ids = tile_ids % tiles_dev
    tile_col = 4 * (owner_ids % block_cols) + local_ids % 4
    tile_row = tiles_dev // 4 * (owner_ids // block_cols) + local_ids // 4
    half_width = TILE_COLS * 8.0
    column = (tile_col[:, None] * 16 + pixel_ids[None, :] % 16).astype(jnp.float32)
    row_pos = (tile_row[:, None] * 16 + pixel_ids[None, :] // 16).astype(jnp.float32)
    return ((column + 0.5 - half_width) / half_width, (row_pos + 0.5 - rows_pix * 0.5) / half_width)


def adam_update(params, first_moment, second_moment, gradient, counts):
    row_ids = lax.broadcasted_iota(jnp.int32, params.shape, 0)
    rates = jnp.where(
        row_ids < 6,
        0.01,
        jnp.where(
            row_ids < 10,
            0.005,
            jnp.where(row_ids < 11, 0.05, jnp.where(row_ids < 14, 0.0025, 0.000125)),
        ),
    )
    first_new = 0.9 * first_moment + 0.1 * gradient
    second = 0.999 * second_moment + 0.001 * gradient * gradient
    bias_one = 1.0 - 0.9**ADAM_STEP
    bias_two = 1.0 - 0.999**ADAM_STEP
    stride = rates * (first_new / bias_one) / (jnp.sqrt(second / bias_two) + 1e-08)
    seen_mask = counts > 0.0
    return (
        jnp.where(seen_mask, params - stride, params),
        jnp.where(seen_mask, first_new, first_moment),
        jnp.where(seen_mask, second, second_moment),
    )


def shards(params, first_moment, second_moment, cameras, visible, send_plan, tile_lists, target):
    cells = lax.axis_size("cells")
    camera = cameras[0]
    plan_rows = send_plan[0, 0]
    capacity = plan_rows.shape[1]
    sent_live = (plan_rows >= 0)[None]
    sent_rows = jnp.maximum(plan_rows, 0)
    lists = tile_lists[0]
    tiles_here = lists.shape[0]
    live_mask = (lists >= 0).astype(jnp.float32)
    slot_ids = jnp.maximum(lists, 0)
    rows_pix = tiles_here * cells // TILE_COLS * 16
    pixel_column, pixel_row = pixel_grid(
        lax.axis_index("cells") * tiles_here, tiles_here, tiles_here, rows_pix
    )
    target_tile = target[0].reshape(3, tiles_here, 256)
    block = params.shape[1]

    def image_loss(table):
        picked = jnp.take(table, slot_ids, axis=1)
        return render_tiles(picked, live_mask, pixel_column, pixel_row, target_tile)

    def own_projection(values):
        return project(values, camera)

    features, project_pull = jax.vjp(own_projection, params)
    outgoing = jnp.take(features, sent_rows, axis=1)
    incoming = lax.all_to_all(outgoing, "cells", split_axis=1, concat_axis=1, tiled=True)
    loss_value, pullback = jax.vjp(
        image_loss, incoming.reshape(features.shape[0], cells * capacity)
    )
    table_grad = pullback(jnp.ones((), jnp.float32))[0]
    returned = lax.all_to_all(
        table_grad.reshape(features.shape[0], cells, capacity),
        "cells",
        split_axis=1,
        concat_axis=1,
        tiled=True,
    )
    kept = jnp.where(sent_live, returned, 0.0)
    gradient = project_pull(
        jnp.zeros((features.shape[0], block), jnp.float32).at[:, sent_rows].add(kept)
    )[0]
    seen_here = visible.astype(jnp.float32)
    total_grad, counts = lax.psum((gradient, seen_here), "views")
    new_params, new_first, new_second = adam_update(
        params, first_moment, second_moment, total_grad, counts
    )
    return (new_params, new_first, new_second)

LANES = 128
PAD_ROWS = 64
FEATS = 9


def project_rows(rows, turn, centre):
    offset = [rows[i] - centre[i] for i in range(3)]
    in_view = [
        turn[i][0] * offset[0] + turn[i][1] * offset[1] + turn[i][2] * offset[2] for i in range(3)
    ]
    inv_depth = 1.0 / in_view[2]
    screen_col = in_view[0] * inv_depth
    screen_row = in_view[1] * inv_depth
    scales = [jnp.exp(rows[3 + i]) for i in range(3)]
    raw = rows[6:10]
    norm = jnp.sqrt(raw[0] * raw[0] + raw[1] * raw[1] + raw[2] * raw[2] + raw[3] * raw[3])
    inv_norm = 1.0 / norm
    quat_w, quat_x, quat_y, quat_z = [item * inv_norm for item in raw]
    spin = [
        [
            1.0 - 2.0 * (quat_y * quat_y + quat_z * quat_z),
            2.0 * (quat_x * quat_y - quat_w * quat_z),
            2.0 * (quat_x * quat_z + quat_w * quat_y),
        ],
        [
            2.0 * (quat_x * quat_y + quat_w * quat_z),
            1.0 - 2.0 * (quat_x * quat_x + quat_z * quat_z),
            2.0 * (quat_y * quat_z - quat_w * quat_x),
        ],
        [
            2.0 * (quat_x * quat_z - quat_w * quat_y),
            2.0 * (quat_y * quat_z + quat_w * quat_x),
            1.0 - 2.0 * (quat_x * quat_x + quat_y * quat_y),
        ],
    ]
    basis_cam = [
        [
            (turn[i][0] * spin[0][j] + turn[i][1] * spin[1][j] + turn[i][2] * spin[2][j])
            * scales[j]
            for j in range(3)
        ]
        for i in range(3)
    ]
    top = [(basis_cam[0][j] - screen_col * basis_cam[2][j]) * inv_depth for j in range(3)]
    low = [(basis_cam[1][j] - screen_row * basis_cam[2][j]) * inv_depth for j in range(3)]
    sigma_a = top[0] * top[0] + top[1] * top[1] + top[2] * top[2]
    sigma_b = top[0] * low[0] + top[1] * low[1] + top[2] * low[2]
    sigma_c = low[0] * low[0] + low[1] * low[1] + low[2] * low[2]
    inv_det = 1.0 / (sigma_a * sigma_c - sigma_b * sigma_b)
    opacity = 1.0 / (1.0 + jnp.exp(-rows[10]))
    inv_dist = 1.0 / jnp.sqrt(offset[0] * offset[0] + offset[1] * offset[1] + offset[2] * offset[2])
    x, y, z = [item * inv_dist for item in offset]
    xx, yy, zz = x * x, y * y, z * z
    basis = [
        None,
        -harmonic_one * y,
        harmonic_one * z,
        -harmonic_one * x,
        harmonic_two[0] * x * y,
        harmonic_two[1] * y * z,
        harmonic_two[2] * (2.0 * zz - xx - yy),
        harmonic_two[3] * x * z,
        harmonic_two[4] * (xx - yy),
        harmonic_three[0] * y * (3.0 * xx - yy),
        harmonic_three[1] * x * y * z,
        harmonic_three[2] * y * (4.0 * zz - xx - yy),
        harmonic_three[3] * z * (2.0 * zz - 3.0 * xx - 3.0 * yy),
        harmonic_three[4] * x * (4.0 * zz - xx - yy),
        harmonic_three[5] * z * (xx - yy),
        harmonic_three[6] * x * (xx - 3.0 * yy),
    ]
    colors = []
    for k in range(3):
        total = harmonic_zero * rows[11 + k]
        for j in range(1, 16):
            total = total + basis[j] * rows[11 + 3 * j + k]
        colors.append(0.5 + total)
    return (
        screen_col,
        screen_row,
        sigma_c * inv_det,
        -sigma_b * inv_det,
        sigma_a * inv_det,
        opacity,
        *colors,
    )


def camera_terms(cam):
    cosines, sines = jnp.cos(cam), jnp.sin(cam)
    cr, cp, cy = [cosines[:, i : i + 1] for i in range(3)]
    sr, sp, sy = [sines[:, i : i + 1] for i in range(3)]
    turn = [
        [cy * cp, cy * sp * sr - sy * cr, cy * sp * cr + sy * sr],
        [sy * cp, sy * sp * sr + cy * cr, sy * sp * cr - cy * sr],
        [-sp, cp * sr, cp * cr],
    ]
    centre = [cam[:, 3 + i : 4 + i] for i in range(3)]
    return turn, centre


def stage_rows(params_ref, staged):
    count, block = params_ref.shape
    for b in range(block // LANES):
        staged[b * PAD_ROWS : b * PAD_ROWS + count, :] = params_ref[:, b * LANES : (b + 1) * LANES]


def lane_pick(source, lanes):
    return jnp.take_along_axis(source, lanes, axis=1, mode="promise_in_bounds")


def gather_eight(load, blocks, index):
    index = jnp.maximum(index, 0)
    lanes, block = index & (LANES - 1), index >> 7
    total = lane_pick(load(0), lanes)
    for b in range(1, blocks):
        total = jnp.where(block == b, lane_pick(load(b), lanes), total)
    return total


def split_three(x):
    first = x.astype(jnp.bfloat16).astype(jnp.float32)
    rest = x - first
    second = rest.astype(jnp.bfloat16).astype(jnp.float32)
    return first, second, rest - second


def scatter_fill(g, index, lhs, hot, start):
    width = g.shape[1]
    parts = jnp.concatenate(split_three(g), axis=0)
    high, low = index >> 7, index & (LANES - 1)
    blocks = lhs.shape[0] // parts.shape[0]
    size = parts.shape[0]
    for b in range(blocks):
        lhs[b * size : (b + 1) * size, pl.ds(start, width)] = jnp.where(
            high == b, parts, 0.0
        ).astype(jnp.bfloat16)
    lane_ids = lax.broadcasted_iota(jnp.int32, (LANES, width), 0)
    hot[:, pl.ds(start, width)] = jnp.where(lane_ids == low, 1.0, 0.0).astype(jnp.bfloat16)


def scatter_finish(lhs, hot):
    out = lax.dot_general(
        lhs[...], hot[...], (((1,), (1,)), ((), ())), preferred_element_type=jnp.float32
    )
    blocks = lhs.shape[0] // 48
    return [
        out[48 * b : 48 * b + 16] + out[48 * b + 16 : 48 * b + 32] + out[48 * b + 32 : 48 * b + 48]
        for b in range(blocks)
    ]


def project_kernel(params_ref, cam_ref, plan_ref, out_ref, staged, table, last, order):
    count, block = params_ref.shape
    blocks = block // LANES
    halves = plan_ref.shape[1] // LANES
    stage_rows(params_ref, staged)
    turn, centre = camera_terms(cam_ref[...])
    for part in range(blocks // 8):
        base = part * 8 * PAD_ROWS
        rows = [staged[pl.ds(base + r, 8, stride=PAD_ROWS), :] for r in range(count)]
        feats = project_rows(rows, turn, centre)
        for f in range(8):
            table[pl.ds(part * 64 + f, 8, stride=8), :] = feats[f]
        last[part * 8 : part * 8 + 8, :] = feats[8]
    slots = plan_ref.shape[0] * halves
    for o in range(slots):
        d, h = divmod(o, halves)
        row = plan_ref[d : d + 1, h * LANES : (h + 1) * LANES]
        order[o : o + 1, :] = row
        out_ref[d, 8 * h : 8 * h + 8, :] = gather_eight(
            lambda b: table[8 * b : 8 * b + 8, :], blocks, jnp.broadcast_to(row, (8, LANES))
        )
    for p in range(slots // 8):
        picked = gather_eight(
            lambda b: jnp.broadcast_to(last[b : b + 1, :], (8, LANES)),
            blocks,
            order[8 * p : 8 * p + 8, :],
        )
        for i in range(8 // halves):
            out_ref[8 // halves * p + i, 8 * halves :, :] = picked[i * halves : (i + 1) * halves]


def exchange_kernel(axis, size, spread, src_ref, dst_ref, send_sem, recv_sem, own_sem):
    me = lax.axis_index(axis)
    barrier = pltpu.get_barrier_semaphore()
    for k in range(1, size):
        pl.semaphore_signal(
            barrier,
            inc=1,
            device_id={axis: lax.rem(me + k, size)},
            device_id_type=pl.DeviceIdType.MESH,
        )
    mine = pltpu.make_async_copy(src_ref.at[me] if spread else src_ref, dst_ref.at[me], own_sem)
    mine.start()
    pl.semaphore_wait(barrier, size - 1)
    copies = []
    for k in range(1, size):
        peer = lax.rem(me + k, size)
        copy = pltpu.make_async_remote_copy(
            src_ref=src_ref.at[peer] if spread else src_ref,
            dst_ref=dst_ref.at[me],
            send_sem=send_sem.at[k - 1],
            recv_sem=recv_sem.at[k - 1],
            device_id={axis: peer},
            device_id_type=pl.DeviceIdType.MESH,
        )
        copy.start()
        copies.append(copy)
    mine.wait()
    for copy in copies:
        copy.wait()


def exchange(x, axis, spread, collective):
    size = lax.axis_size(axis)
    shape = x.shape if spread else (size,) + x.shape
    return pl.pallas_call(
        functools.partial(exchange_kernel, axis, size, spread),
        out_shape=jax.ShapeDtypeStruct(shape, x.dtype),
        in_specs=[pl.BlockSpec(memory_space=pltpu.VMEM)],
        out_specs=pl.BlockSpec(memory_space=pltpu.VMEM),
        scratch_shapes=[
            pltpu.SemaphoreType.DMA((size - 1,)),
            pltpu.SemaphoreType.DMA((size - 1,)),
            pltpu.SemaphoreType.DMA,
        ],
        compiler_params=pltpu.CompilerParams(collective_id=collective, has_side_effects=True),
    )(x)


def render_kernel(
    cells, recv_ref, lists_ref, target_ref, out_ref,
    order, picks, wanted, before, after, alpha_s, trans_s, flow_s, parts_s, pair_s, lhs, hot,
):
    tiles, entries = lists_ref.shape
    owners, packed, _ = recv_ref.shape
    halves = packed // FEATS
    blocks = owners * halves
    quarters = entries // LANES
    me = lax.axis_index("cells")
    rows_pix = tiles * cells // TILE_COLS * 16
    half_width = TILE_COLS * 8.0
    wanted[...] = jnp.transpose(
        jnp.concatenate([target_ref[...], jnp.zeros((5, target_ref.shape[1]), jnp.float32)], axis=0)
    )
    row_ids = lax.broadcasted_iota(jnp.int32, (entries, entries), 0)
    col_ids = lax.broadcasted_iota(jnp.int32, (entries, entries), 1)
    before[...] = jnp.where(row_ids < col_ids, 1.0, 0.0).astype(jnp.bfloat16)
    after[...] = jnp.where(row_ids > col_ids, 1.0, 0.0).astype(jnp.bfloat16)

    def load_main(b):
        s, h = divmod(b, halves)
        return recv_ref[s, 8 * h : 8 * h + 8, :]

    def load_last(b):
        s, h = divmod(b, halves)
        return jnp.broadcast_to(recv_ref[s, 8 * halves + h : 8 * halves + h + 1, :], (8, LANES))

    slots = tiles * quarters
    for o in range(slots):
        t, q = divmod(o, quarters)
        row = lists_ref[t : t + 1, q * LANES : (q + 1) * LANES]
        order[o : o + 1, :] = row
        picks[t, 0:8, q * LANES : (q + 1) * LANES] = gather_eight(
            load_main, blocks, jnp.broadcast_to(row, (8, LANES))
        )
    for p in range(slots // 8):
        picked = gather_eight(load_last, blocks, order[8 * p : 8 * p + 8, :])
        for i in range(8):
            t, q = divmod(8 * p + i, quarters)
            picks[t, 8:9, q * LANES : (q + 1) * LANES] = picked[i : i + 1]

    def one_tile(t, carry):
        def feature(f):
            return picks[t, f : f + 1, :]

        listed = lists_ref[pl.ds(t, 1), :]
        opacity = jnp.where(listed >= 0, feature(5), 0.0)
        tile_col = 4 * lax.rem(me, TILE_COLS // 4) + lax.rem(t, 4)
        tile_row = tiles // 4 * lax.div(me, TILE_COLS // 4) + lax.div(t, 4)
        across = (lax.broadcasted_iota(jnp.int32, (16, entries), 0) + tile_col * 16).astype(jnp.float32)
        delta_col = (across + 0.5 - half_width) * (1.0 / half_width) - feature(0)
        square_term = -0.5 * feature(2) * delta_col * delta_col
        cross_term = -feature(3) * delta_col
        row_scale = -0.5 * feature(4)

        def delta_row_at(r):
            down = (jnp.full((1, entries), tile_row * 16 + r, jnp.int32)).astype(jnp.float32)
            return (down + 0.5 - rows_pix * 0.5) * (1.0 / half_width) - feature(1)

        def put_parts(r, x):
            first = x.astype(jnp.bfloat16)
            parts_s[pl.ds(r * 16, 16), :] = first
            parts_s[pl.ds(256 + r * 16, 16), :] = (x - first.astype(jnp.float32)).astype(jnp.bfloat16)

        def forward(r, carry):
            delta_row = delta_row_at(r)
            power = square_term + cross_term * delta_row + row_scale * delta_row * delta_row
            alpha = opacity * jnp.exp(power)
            alpha_s[pl.ds(r * 16, 16), :] = alpha
            put_parts(r, jnp.log(1.0 - alpha))
            return carry

        lax.fori_loop(0, 16, forward, 0, unroll=2)
        sums = jnp.dot(parts_s[...], before[...], preferred_element_type=jnp.float32)
        trans_s[...] = jnp.exp(sums[0:256] + sums[256:512])

        def colors_of(r, carry):
            weight = alpha_s[pl.ds(r * 16, 16), :] * trans_s[pl.ds(r * 16, 16), :]
            goal = wanted[pl.ds(t * 256 + r * 16, 16), :]
            slope = 0.0
            sums = []
            for k in range(3):
                value = jnp.sum(weight * feature(6 + k), axis=1, keepdims=True)
                error = 2.0 * (value - goal[:, k : k + 1])
                slope = slope + error * feature(6 + k)
                sums.append(carry[k] + error * weight)
            flow = weight * slope
            flow_s[pl.ds(r * 16, 16), :] = flow
            put_parts(r, flow)
            return tuple(sums)

        empty = jnp.zeros((16, entries), jnp.float32)
        color_sums = lax.fori_loop(0, 16, colors_of, (empty, empty, empty))
        sums = jnp.dot(parts_s[...], after[...], preferred_element_type=jnp.float32)
        trans_s[...] = sums[0:256] + sums[256:512]

        def backward(r, carry):
            delta_row = delta_row_at(r)
            alpha = alpha_s[pl.ds(r * 16, 16), :]
            slope = flow_s[pl.ds(r * 16, 16), :] - alpha / (1.0 - alpha) * trans_s[pl.ds(r * 16, 16), :]
            return (
                carry[0] + slope,
                carry[1] + slope * delta_row,
                carry[2] + slope * (delta_row * delta_row),
            )

        plain, tilted, bent = lax.fori_loop(0, 16, backward, (empty, empty, empty), unroll=2)

        def fold(x):
            return jnp.sum(x, axis=0, keepdims=True)

        moved = plain * delta_col
        pair_s[...] = jnp.concatenate(
            [
                fold(plain),
                fold(moved),
                fold(tilted),
                fold(moved * delta_col),
                fold(tilted * delta_col),
                fold(bent),
                fold(color_sums[0]),
                fold(color_sums[1]),
                fold(color_sums[2]),
                jnp.zeros((7, entries), jnp.float32),
            ],
            axis=0,
        )
        scatter_fill(pair_s[...], listed, lhs, hot, pl.multiple_of(t * entries, entries))
        return carry

    lax.fori_loop(0, tiles, one_tile, 0)
    for b, piece in enumerate(scatter_finish(lhs, hot)):
        s, h = divmod(b, halves)
        out_ref[s, 8 * h : 8 * h + 8, :] = piece[0:8]
        out_ref[s, 8 * halves + h : 8 * halves + h + 1, :] = piece[8:9]


def owner_kernel(back_ref, plan_ref, visible_ref, cam_ref, out_ref, lhs, hot, spread):
    devices, packed, _ = back_ref.shape
    halves = packed // FEATS
    for d in range(devices):
        main = jnp.concatenate([back_ref[d, 8 * h : 8 * h + 8, :] for h in range(halves)], axis=1)
        last = jnp.concatenate(
            [back_ref[d, 8 * halves + h : 8 * halves + h + 1, :] for h in range(halves)], axis=1
        )
        g = jnp.concatenate([main, last, jnp.zeros((7, halves * LANES), jnp.float32)], axis=0)
        scatter_fill(g, plan_ref[d : d + 1, :], lhs, hot, d * halves * LANES)
    pieces = scatter_finish(lhs, hot)
    blocks = len(pieces)
    for b, piece in enumerate(pieces):
        spread[16 * b : 16 * b + 16, :] = piece
    for f in range(FEATS):
        out_ref[f] = spread[pl.ds(f, blocks, stride=16), :]
    for b in range(blocks):
        out_ref[FEATS, b : b + 1, :] = visible_ref[:, b * LANES : (b + 1) * LANES].astype(jnp.float32)
    out_ref[FEATS + 1] = jnp.broadcast_to(
        jnp.concatenate([cam_ref[...], jnp.zeros((1, LANES - 6), jnp.float32)], axis=1),
        (blocks, LANES),
    )


def update_kernel(params_ref, first_ref, second_ref, shared_ref, new_ref, new_first_ref, new_second_ref, staged, grads):
    count, block = params_ref.shape
    blocks = block // LANES
    views = shared_ref.shape[0]
    stage_rows(params_ref, staged)
    grads[...] = jnp.zeros_like(grads)

    def one_part(step, carry):
        part, view = lax.div(step, views), lax.rem(step, views)
        base = part * (8 * PAD_ROWS)
        start = pl.multiple_of(part * 8, 8)
        cam = shared_ref[view, FEATS + 1, 0:1, :]
        turn, centre = camera_terms(cam)
        rows = tuple(staged[pl.ds(base + r, 8, stride=PAD_ROWS), :] for r in range(count))
        feats, pull = jax.vjp(lambda *items: project_rows(items, turn, centre), *rows)
        got = [shared_ref[view, f, pl.ds(start, 8), :] for f in range(FEATS)]
        slopes = (
            feats[2] * got[1] + feats[3] * got[2],
            feats[3] * got[1] + feats[4] * got[2],
            -0.5 * got[3],
            -got[4],
            -0.5 * got[5],
            got[0] / feats[5],
            got[6],
            got[7],
            got[8],
        )
        for r, item in enumerate(pull(slopes)):
            where = pl.ds(base + r, 8, stride=PAD_ROWS)
            grads[where, :] = grads[where, :] + item
        return carry

    lax.fori_loop(0, blocks // 8 * views, one_part, 0)
    row_ids = lax.broadcasted_iota(jnp.int32, (count, LANES), 0)
    rates = jnp.where(
        row_ids < 6,
        0.01,
        jnp.where(
            row_ids < 10,
            0.005,
            jnp.where(row_ids < 11, 0.05, jnp.where(row_ids < 14, 0.0025, 0.000125)),
        ),
    )
    bias_one = 1.0 - 0.9**ADAM_STEP
    bias_two = 1.0 - 0.999**ADAM_STEP
    for b in range(blocks):
        span = slice(b * LANES, (b + 1) * LANES)
        gradient = grads[b * PAD_ROWS : b * PAD_ROWS + count, :]
        params, first, second = params_ref[:, span], first_ref[:, span], second_ref[:, span]
        counts = shared_ref[0, FEATS, b : b + 1, :]
        for view in range(1, views):
            counts = counts + shared_ref[view, FEATS, b : b + 1, :]
        seen = jnp.broadcast_to(counts, params.shape) > 0.0
        first_new = 0.9 * first + 0.1 * gradient
        second_new = 0.999 * second + 0.001 * gradient * gradient
        stride = rates * (first_new / bias_one) / (jnp.sqrt(second_new / bias_two) + 1e-08)
        new_ref[:, span] = jnp.where(seen, params - stride, params)
        new_first_ref[:, span] = jnp.where(seen, first_new, first)
        new_second_ref[:, span] = jnp.where(seen, second_new, second)


def fused_shards(params, first_moment, second_moment, cameras, visible, send_plan, tile_lists, target):
    cells = lax.axis_size("cells")
    count, block = params.shape
    blocks = block // LANES
    plan = send_plan[0, 0]
    lists = tile_lists[0]
    tiles, entries = lists.shape
    halves = plan.shape[1] // LANES
    slots = cells * halves
    f32, bf16 = jnp.float32, jnp.bfloat16
    packet = jax.ShapeDtypeStruct((cells, FEATS * halves, LANES), f32)
    outgoing = pl.pallas_call(
        project_kernel,
        out_shape=packet,
        scratch_shapes=[
            pltpu.VMEM((blocks * PAD_ROWS, LANES), f32),
            pltpu.VMEM((blocks * 8, LANES), f32),
            pltpu.VMEM((blocks, LANES), f32),
            pltpu.VMEM((slots, LANES), jnp.int32),
        ],
    )(params, cameras, plan)
    incoming = exchange(outgoing, "cells", True, 0)
    back = pl.pallas_call(
        functools.partial(render_kernel, cells),
        out_shape=packet,
        scratch_shapes=[
            pltpu.VMEM((tiles * entries // LANES, LANES), jnp.int32),
            pltpu.VMEM((tiles, 16, entries), f32),
            pltpu.VMEM((tiles * 256, 8), f32),
            pltpu.VMEM((entries, entries), bf16),
            pltpu.VMEM((entries, entries), bf16),
            pltpu.VMEM((256, entries), f32),
            pltpu.VMEM((256, entries), f32),
            pltpu.VMEM((256, entries), f32),
            pltpu.VMEM((512, entries), bf16),
            pltpu.VMEM((16, entries), f32),
            pltpu.VMEM((slots * 48, tiles * entries), bf16),
            pltpu.VMEM((LANES, tiles * entries), bf16),
        ],
    )(incoming, lists, target[0])
    returned = exchange(back, "cells", True, 1)
    mine = pl.pallas_call(
        owner_kernel,
        out_shape=jax.ShapeDtypeStruct((FEATS + 2, blocks, LANES), f32),
        scratch_shapes=[
            pltpu.VMEM((blocks * 48, slots * LANES), bf16),
            pltpu.VMEM((LANES, slots * LANES), bf16),
            pltpu.VMEM((blocks * 16, LANES), f32),
        ],
    )(returned, plan, visible, cameras)
    shared = exchange(mine, "views", False, 2)
    like = jax.ShapeDtypeStruct(params.shape, f32)
    return tuple(
        pl.pallas_call(
            update_kernel,
            out_shape=(like, like, like),
            scratch_shapes=[
                pltpu.VMEM((blocks * PAD_ROWS, LANES), f32),
                pltpu.VMEM((blocks * PAD_ROWS, LANES), f32),
            ],
        )(params, first_moment, second_moment, shared)
    )


def local_shards(params, first_moment, second_moment, cameras, visible, send_plan, tile_lists, target):
    capacity = send_plan.shape[3]
    tiles, entries = tile_lists.shape[1:]
    halves = capacity // LANES
    fits = (
        capacity % LANES == 0
        and params.shape[1] % (8 * LANES) == 0
        and entries % LANES == 0
        and 8 % max(halves, 1) == 0
        and lax.axis_size("cells") * halves % 8 == 0
        and tiles * entries // LANES % 8 == 0
        and tiles * entries <= 4096
        and tiles % 4 == 0
    )
    body = fused_shards if fits else shards
    return body(params, first_moment, second_moment, cameras, visible, send_plan, tile_lists, target)


def solution(mesh):
    in_specs = (
        P(None, "cells"),
        P(None, "cells"),
        P(None, "cells"),
        P("views", None),
        P("views", "cells"),
        P("views", "cells", None, None),
        P("views", "cells", None),
        P("views", None, "cells"),
    )
    out_specs = (P(None, "cells"), P(None, "cells"), P(None, "cells"))
    return jax.shard_map(local_shards, mesh=mesh, in_specs=in_specs, out_specs=out_specs, check_vma=False)
```

```python
import functools

import jax
import jax.numpy as jnp
from jax import lax
from jax.experimental import pallas as pl
from jax.experimental.pallas import tpu as pltpu
from jax.sharding import PartitionSpec as P

TILE_COLS = 32
ADAM_STEP = 1000


harmonic_zero = 0.28209479177387814
harmonic_one = 0.4886025119029199
harmonic_two = (
    1.0925484305920792,
    -1.0925484305920792,
    0.31539156525252005,
    -1.0925484305920792,
    0.5462742152960396,
)
harmonic_three = (
    -0.5900435899266435,
    2.890611442640554,
    -0.4570457994644658,
    0.3731763325901154,
    -0.4570457994644658,
    1.445305721320277,
    -0.5900435899266435,
)


def harmonics(across, upward, onward):
    across_sq = across * across
    upward_sq = upward * upward
    onward_sq = onward * onward
    return jnp.stack(
        [
            harmonic_zero * jnp.ones_like(across),
            -harmonic_one * upward,
            harmonic_one * onward,
            -harmonic_one * across,
            harmonic_two[0] * across * upward,
            harmonic_two[1] * upward * onward,
            harmonic_two[2] * (2.0 * onward_sq - across_sq - upward_sq),
            harmonic_two[3] * across * onward,
            harmonic_two[4] * (across_sq - upward_sq),
            harmonic_three[0] * upward * (3.0 * across_sq - upward_sq),
            harmonic_three[1] * across * upward * onward,
            harmonic_three[2] * upward * (4.0 * onward_sq - across_sq - upward_sq),
            harmonic_three[3] * onward * (2.0 * onward_sq - 3.0 * across_sq - 3.0 * upward_sq),
            harmonic_three[4] * across * (4.0 * onward_sq - across_sq - upward_sq),
            harmonic_three[5] * onward * (across_sq - upward_sq),
            harmonic_three[6] * across * (across_sq - 3.0 * upward_sq),
        ]
    )


def camera_rotation(angles):
    cos_roll, sin_roll = (jnp.cos(angles[0]), jnp.sin(angles[0]))
    cos_pitch, sin_pitch = (jnp.cos(angles[1]), jnp.sin(angles[1]))
    cos_yaw, sin_yaw = (jnp.cos(angles[2]), jnp.sin(angles[2]))
    naught = jnp.zeros_like(cos_roll)
    unit_one = jnp.ones_like(cos_roll)
    roll = jnp.stack(
        [
            jnp.stack([unit_one, naught, naught]),
            jnp.stack([naught, cos_roll, -sin_roll]),
            jnp.stack([naught, sin_roll, cos_roll]),
        ]
    )
    pitch = jnp.stack(
        [
            jnp.stack([cos_pitch, naught, sin_pitch]),
            jnp.stack([naught, unit_one, naught]),
            jnp.stack([-sin_pitch, naught, cos_pitch]),
        ]
    )
    yawing = jnp.stack(
        [
            jnp.stack([cos_yaw, -sin_yaw, naught]),
            jnp.stack([sin_yaw, cos_yaw, naught]),
            jnp.stack([naught, naught, unit_one]),
        ]
    )
    inner_turn = jnp.dot(pitch, roll, precision=lax.Precision.HIGHEST)
    return jnp.dot(yawing, inner_turn, precision=lax.Precision.HIGHEST)


def project(values, camera):
    turn = camera_rotation(camera[0:3])
    offset = values[0:3] - camera[3:6][:, None]
    in_view = jnp.dot(turn, offset, precision=lax.Precision.HIGHEST)
    inv_depth = 1.0 / in_view[2]
    screen_col = in_view[0] * inv_depth
    screen_row = in_view[1] * inv_depth
    scales = jnp.exp(values[3:6])
    quat = values[6:10] / jnp.sqrt(jnp.sum(values[6:10] * values[6:10], axis=0, keepdims=True))
    quat_w, quat_x, quat_y, quat_z = (quat[0], quat[1], quat[2], quat[3])
    spin = [
        [
            1.0 - 2.0 * (quat_y * quat_y + quat_z * quat_z),
            2.0 * (quat_x * quat_y - quat_w * quat_z),
            2.0 * (quat_x * quat_z + quat_w * quat_y),
        ],
        [
            2.0 * (quat_x * quat_y + quat_w * quat_z),
            1.0 - 2.0 * (quat_x * quat_x + quat_z * quat_z),
            2.0 * (quat_y * quat_z - quat_w * quat_x),
        ],
        [
            2.0 * (quat_x * quat_z - quat_w * quat_y),
            2.0 * (quat_y * quat_z + quat_w * quat_x),
            1.0 - 2.0 * (quat_x * quat_x + quat_y * quat_y),
        ],
    ]
    basis_cam = []
    for outer_index in range(3):
        row_terms = []
        for col_index in range(3):
            entry = turn[outer_index, 0] * spin[0][col_index]
            for mid_index in range(1, 3):
                entry = entry + turn[outer_index, mid_index] * spin[mid_index][col_index]
            row_terms.append(entry * scales[col_index])
        basis_cam.append(row_terms)
    jac_top = [
        (basis_cam[0][col_index] - screen_col * basis_cam[2][col_index]) * inv_depth
        for col_index in range(3)
    ]
    jac_low = [
        (basis_cam[1][col_index] - screen_row * basis_cam[2][col_index]) * inv_depth
        for col_index in range(3)
    ]
    sigma_a = jac_top[0] * jac_top[0] + jac_top[1] * jac_top[1] + jac_top[2] * jac_top[2]
    sigma_b = jac_top[0] * jac_low[0] + jac_top[1] * jac_low[1] + jac_top[2] * jac_low[2]
    sigma_c = jac_low[0] * jac_low[0] + jac_low[1] * jac_low[1] + jac_low[2] * jac_low[2]
    determinant = sigma_a * sigma_c - sigma_b * sigma_b
    opacity = jax.nn.sigmoid(values[10])
    distance = jnp.sqrt(jnp.sum(offset * offset, axis=0))
    unit_dir = offset / distance
    basis = harmonics(unit_dir[0], unit_dir[1], unit_dir[2])
    coeffs = values[11:59].reshape(16, 3, values.shape[1])
    colors = 0.5 + jnp.sum(basis[:, None, :] * coeffs, axis=0)
    screen = jnp.stack(
        [
            screen_col,
            screen_row,
            sigma_c / determinant,
            -sigma_b / determinant,
            sigma_a / determinant,
            opacity,
        ]
    )
    return jnp.concatenate([screen, colors], axis=0)


def group_loss(pieces):
    features, live_mask, pixel_column, pixel_row, target_tile = pieces
    entries = live_mask.shape[1]
    delta_col = pixel_column[:, :, None] - features[0][:, None, :]
    delta_row = pixel_row[:, :, None] - features[1][:, None, :]
    power = -0.5 * (
        features[2][:, None, :] * delta_col * delta_col
        + 2.0 * features[3][:, None, :] * delta_col * delta_row
        + features[4][:, None, :] * delta_row * delta_row
    )
    alphas = features[5][:, None, :] * jnp.exp(power) * live_mask[:, None, :]
    log_keep = jnp.log(1.0 - alphas)
    earlier = (
        lax.broadcasted_iota(jnp.int32, (entries, entries), 0)
        < lax.broadcasted_iota(jnp.int32, (entries, entries), 1)
    ).astype(jnp.float32)
    transmit = jnp.exp(
        jnp.einsum("bpl,lm->bpm", log_keep, earlier, precision=lax.Precision.HIGHEST)
    )
    weights = alphas * transmit
    image = jnp.einsum("bpl,kbl->kbp", weights, features[6:9], precision=lax.Precision.HIGHEST)
    error = image - target_tile
    return jnp.sum(error * error)


def render_tiles(picked, live_mask, pixel_column, pixel_row, target_tile):
    groups = live_mask.shape[0] // 4
    entries = live_mask.shape[1]
    pixels = pixel_column.shape[1]
    stacked = (
        jnp.transpose(picked.reshape(picked.shape[0], groups, 4, entries), (1, 0, 2, 3)),
        live_mask.reshape(groups, 4, entries),
        pixel_column.reshape(groups, 4, pixels),
        pixel_row.reshape(groups, 4, pixels),
        jnp.transpose(target_tile.reshape(3, groups, 4, pixels), (1, 0, 2, 3)),
    )
    return jnp.sum(lax.map(jax.checkpoint(group_loss), stacked))


def pixel_grid(first_tile, count, tiles_dev, rows_pix):
    tile_ids = first_tile + jnp.arange(count, dtype=jnp.int32)
    pixel_ids = jnp.arange(256, dtype=jnp.int32)
    block_cols = TILE_COLS // 4
    owner_ids = tile_ids // tiles_dev
    local_ids = tile_ids % tiles_dev
    tile_col = 4 * (owner_ids % block_cols) + local_ids % 4
    tile_row = tiles_dev // 4 * (owner_ids // block_cols) + local_ids // 4
    half_width = TILE_COLS * 8.0
    column = (tile_col[:, None] * 16 + pixel_ids[None, :] % 16).astype(jnp.float32)
    row_pos = (tile_row[:, None] * 16 + pixel_ids[None, :] // 16).astype(jnp.float32)
    return ((column + 0.5 - half_width) / half_width, (row_pos + 0.5 - rows_pix * 0.5) / half_width)


def adam_update(params, first_moment, second_moment, gradient, counts):
    row_ids = lax.broadcasted_iota(jnp.int32, params.shape, 0)
    rates = jnp.where(
        row_ids < 6,
        0.01,
        jnp.where(
            row_ids < 10,
            0.005,
            jnp.where(row_ids < 11, 0.05, jnp.where(row_ids < 14, 0.0025, 0.000125)),
        ),
    )
    first_new = 0.9 * first_moment + 0.1 * gradient
    second = 0.999 * second_moment + 0.001 * gradient * gradient
    bias_one = 1.0 - 0.9**ADAM_STEP
    bias_two = 1.0 - 0.999**ADAM_STEP
    stride = rates * (first_new / bias_one) / (jnp.sqrt(second / bias_two) + 1e-08)
    seen_mask = counts > 0.0
    return (
        jnp.where(seen_mask, params - stride, params),
        jnp.where(seen_mask, first_new, first_moment),
        jnp.where(seen_mask, second, second_moment),
    )


def shards(params, first_moment, second_moment, cameras, visible, send_plan, tile_lists, target):
    cells = lax.axis_size("cells")
    camera = cameras[0]
    plan_rows = send_plan[0, 0]
    capacity = plan_rows.shape[1]
    sent_live = (plan_rows >= 0)[None]
    sent_rows = jnp.maximum(plan_rows, 0)
    lists = tile_lists[0]
    tiles_here = lists.shape[0]
    live_mask = (lists >= 0).astype(jnp.float32)
    slot_ids = jnp.maximum(lists, 0)
    rows_pix = tiles_here * cells // TILE_COLS * 16
    pixel_column, pixel_row = pixel_grid(
        lax.axis_index("cells") * tiles_here, tiles_here, tiles_here, rows_pix
    )
    target_tile = target[0].reshape(3, tiles_here, 256)
    block = params.shape[1]

    def image_loss(table):
        picked = jnp.take(table, slot_ids, axis=1)
        return render_tiles(picked, live_mask, pixel_column, pixel_row, target_tile)

    def own_projection(values):
        return project(values, camera)

    features, project_pull = jax.vjp(own_projection, params)
    outgoing = jnp.take(features, sent_rows, axis=1)
    incoming = lax.all_to_all(outgoing, "cells", split_axis=1, concat_axis=1, tiled=True)
    loss_value, pullback = jax.vjp(
        image_loss, incoming.reshape(features.shape[0], cells * capacity)
    )
    table_grad = pullback(jnp.ones((), jnp.float32))[0]
    returned = lax.all_to_all(
        table_grad.reshape(features.shape[0], cells, capacity),
        "cells",
        split_axis=1,
        concat_axis=1,
        tiled=True,
    )
    kept = jnp.where(sent_live, returned, 0.0)
    gradient = project_pull(
        jnp.zeros((features.shape[0], block), jnp.float32).at[:, sent_rows].add(kept)
    )[0]
    seen_here = visible.astype(jnp.float32)
    total_grad, counts = lax.psum((gradient, seen_here), "views")
    new_params, new_first, new_second = adam_update(
        params, first_moment, second_moment, total_grad, counts
    )
    return (new_params, new_first, new_second)

LANES = 128
PAD_ROWS = 64
FEATS = 9


def project_rows(rows, turn, centre):
    offset = [rows[i] - centre[i] for i in range(3)]
    in_view = [
        turn[i][0] * offset[0] + turn[i][1] * offset[1] + turn[i][2] * offset[2] for i in range(3)
    ]
    inv_depth = 1.0 / in_view[2]
    screen_col = in_view[0] * inv_depth
    screen_row = in_view[1] * inv_depth
    scales = [jnp.exp(rows[3 + i]) for i in range(3)]
    raw = rows[6:10]
    norm = jnp.sqrt(raw[0] * raw[0] + raw[1] * raw[1] + raw[2] * raw[2] + raw[3] * raw[3])
    inv_norm = 1.0 / norm
    quat_w, quat_x, quat_y, quat_z = [item * inv_norm for item in raw]
    spin = [
        [
            1.0 - 2.0 * (quat_y * quat_y + quat_z * quat_z),
            2.0 * (quat_x * quat_y - quat_w * quat_z),
            2.0 * (quat_x * quat_z + quat_w * quat_y),
        ],
        [
            2.0 * (quat_x * quat_y + quat_w * quat_z),
            1.0 - 2.0 * (quat_x * quat_x + quat_z * quat_z),
            2.0 * (quat_y * quat_z - quat_w * quat_x),
        ],
        [
            2.0 * (quat_x * quat_z - quat_w * quat_y),
            2.0 * (quat_y * quat_z + quat_w * quat_x),
            1.0 - 2.0 * (quat_x * quat_x + quat_y * quat_y),
        ],
    ]
    basis_cam = [
        [
            (turn[i][0] * spin[0][j] + turn[i][1] * spin[1][j] + turn[i][2] * spin[2][j])
            * scales[j]
            for j in range(3)
        ]
        for i in range(3)
    ]
    top = [(basis_cam[0][j] - screen_col * basis_cam[2][j]) * inv_depth for j in range(3)]
    low = [(basis_cam[1][j] - screen_row * basis_cam[2][j]) * inv_depth for j in range(3)]
    sigma_a = top[0] * top[0] + top[1] * top[1] + top[2] * top[2]
    sigma_b = top[0] * low[0] + top[1] * low[1] + top[2] * low[2]
    sigma_c = low[0] * low[0] + low[1] * low[1] + low[2] * low[2]
    inv_det = 1.0 / (sigma_a * sigma_c - sigma_b * sigma_b)
    opacity = 1.0 / (1.0 + jnp.exp(-rows[10]))
    inv_dist = 1.0 / jnp.sqrt(offset[0] * offset[0] + offset[1] * offset[1] + offset[2] * offset[2])
    x, y, z = [item * inv_dist for item in offset]
    xx, yy, zz = x * x, y * y, z * z
    basis = [
        None,
        -harmonic_one * y,
        harmonic_one * z,
        -harmonic_one * x,
        harmonic_two[0] * x * y,
        harmonic_two[1] * y * z,
        harmonic_two[2] * (2.0 * zz - xx - yy),
        harmonic_two[3] * x * z,
        harmonic_two[4] * (xx - yy),
        harmonic_three[0] * y * (3.0 * xx - yy),
        harmonic_three[1] * x * y * z,
        harmonic_three[2] * y * (4.0 * zz - xx - yy),
        harmonic_three[3] * z * (2.0 * zz - 3.0 * xx - 3.0 * yy),
        harmonic_three[4] * x * (4.0 * zz - xx - yy),
        harmonic_three[5] * z * (xx - yy),
        harmonic_three[6] * x * (xx - 3.0 * yy),
    ]
    colors = []
    for k in range(3):
        total = harmonic_zero * rows[11 + k]
        for j in range(1, 16):
            total = total + basis[j] * rows[11 + 3 * j + k]
        colors.append(0.5 + total)
    return (
        screen_col,
        screen_row,
        sigma_c * inv_det,
        -sigma_b * inv_det,
        sigma_a * inv_det,
        opacity,
        *colors,
    )


def camera_terms(cam):
    cosines, sines = jnp.cos(cam), jnp.sin(cam)
    cr, cp, cy = [cosines[:, i : i + 1] for i in range(3)]
    sr, sp, sy = [sines[:, i : i + 1] for i in range(3)]
    turn = [
        [cy * cp, cy * sp * sr - sy * cr, cy * sp * cr + sy * sr],
        [sy * cp, sy * sp * sr + cy * cr, sy * sp * cr - cy * sr],
        [-sp, cp * sr, cp * cr],
    ]
    centre = [cam[:, 3 + i : 4 + i] for i in range(3)]
    return turn, centre


def stage_rows(params_ref, staged):
    count, block = params_ref.shape
    for b in range(block // LANES):
        staged[b * PAD_ROWS : b * PAD_ROWS + count, :] = params_ref[:, b * LANES : (b + 1) * LANES]


def lane_pick(source, lanes):
    return jnp.take_along_axis(source, lanes, axis=1, mode="promise_in_bounds")


def gather_eight(load, blocks, index):
    index = jnp.maximum(index, 0)
    lanes, block = index & (LANES - 1), index >> 7
    total = lane_pick(load(0), lanes)
    for b in range(1, blocks):
        total = jnp.where(block == b, lane_pick(load(b), lanes), total)
    return total


def split_three(x):
    first = x.astype(jnp.bfloat16).astype(jnp.float32)
    rest = x - first
    second = rest.astype(jnp.bfloat16).astype(jnp.float32)
    return first, second, rest - second


def scatter_fill(g, index, lhs, hot, start):
    width = g.shape[1]
    parts = jnp.concatenate(split_three(g), axis=0)
    high, low = index >> 7, index & (LANES - 1)
    blocks = lhs.shape[0] // parts.shape[0]
    size = parts.shape[0]
    for b in range(blocks):
        lhs[b * size : (b + 1) * size, pl.ds(start, width)] = jnp.where(
            high == b, parts, 0.0
        ).astype(jnp.bfloat16)
    lane_ids = lax.broadcasted_iota(jnp.int32, (LANES, width), 0)
    hot[:, pl.ds(start, width)] = jnp.where(lane_ids == low, 1.0, 0.0).astype(jnp.bfloat16)


def scatter_finish(lhs, hot):
    out = lax.dot_general(
        lhs[...], hot[...], (((1,), (1,)), ((), ())), preferred_element_type=jnp.float32
    )
    blocks = lhs.shape[0] // 48
    return [
        out[48 * b : 48 * b + 16] + out[48 * b + 16 : 48 * b + 32] + out[48 * b + 32 : 48 * b + 48]
        for b in range(blocks)
    ]


def project_kernel(params_ref, cam_ref, plan_ref, out_ref, staged, table, last, order):
    count, block = params_ref.shape
    blocks = block // LANES
    halves = plan_ref.shape[1] // LANES
    stage_rows(params_ref, staged)
    turn, centre = camera_terms(cam_ref[...])
    for part in range(blocks // 8):
        base = part * 8 * PAD_ROWS
        rows = [staged[pl.ds(base + r, 8, stride=PAD_ROWS), :] for r in range(count)]
        feats = project_rows(rows, turn, centre)
        for f in range(8):
            table[pl.ds(part * 64 + f, 8, stride=8), :] = feats[f]
        last[part * 8 : part * 8 + 8, :] = feats[8]
    slots = plan_ref.shape[0] * halves
    for o in range(slots):
        d, h = divmod(o, halves)
        row = plan_ref[d : d + 1, h * LANES : (h + 1) * LANES]
        order[o : o + 1, :] = row
        out_ref[d, 8 * h : 8 * h + 8, :] = gather_eight(
            lambda b: table[8 * b : 8 * b + 8, :], blocks, jnp.broadcast_to(row, (8, LANES))
        )
    for p in range(slots // 8):
        picked = gather_eight(
            lambda b: jnp.broadcast_to(last[b : b + 1, :], (8, LANES)),
            blocks,
            order[8 * p : 8 * p + 8, :],
        )
        for i in range(8 // halves):
            out_ref[8 // halves * p + i, 8 * halves :, :] = picked[i * halves : (i + 1) * halves]


def exchange_kernel(axis, size, spread, src_ref, dst_ref, send_sem, recv_sem, own_sem):
    me = lax.axis_index(axis)
    barrier = pltpu.get_barrier_semaphore()
    for k in range(1, size):
        pl.semaphore_signal(
            barrier,
            inc=1,
            device_id={axis: lax.rem(me + k, size)},
            device_id_type=pl.DeviceIdType.MESH,
        )
    mine = pltpu.make_async_copy(src_ref.at[me] if spread else src_ref, dst_ref.at[me], own_sem)
    mine.start()
    pl.semaphore_wait(barrier, size - 1)
    copies = []
    for k in range(1, size):
        peer = lax.rem(me + k, size)
        copy = pltpu.make_async_remote_copy(
            src_ref=src_ref.at[peer] if spread else src_ref,
            dst_ref=dst_ref.at[me],
            send_sem=send_sem.at[k - 1],
            recv_sem=recv_sem.at[k - 1],
            device_id={axis: peer},
            device_id_type=pl.DeviceIdType.MESH,
        )
        copy.start()
        copies.append(copy)
    mine.wait()
    for copy in copies:
        copy.wait()


def exchange(x, axis, spread, collective):
    size = lax.axis_size(axis)
    shape = x.shape if spread else (size,) + x.shape
    return pl.pallas_call(
        functools.partial(exchange_kernel, axis, size, spread),
        out_shape=jax.ShapeDtypeStruct(shape, x.dtype),
        in_specs=[pl.BlockSpec(memory_space=pltpu.VMEM)],
        out_specs=pl.BlockSpec(memory_space=pltpu.VMEM),
        scratch_shapes=[
            pltpu.SemaphoreType.DMA((size - 1,)),
            pltpu.SemaphoreType.DMA((size - 1,)),
            pltpu.SemaphoreType.DMA,
        ],
        compiler_params=pltpu.CompilerParams(collective_id=collective, has_side_effects=True),
    )(x)


def render_kernel(
    cells, recv_ref, lists_ref, target_ref, out_ref,
    order, picks, wanted, before, after, alpha_s, trans_s, flow_s, parts_s, pair_s, lhs, hot,
):
    tiles, entries = lists_ref.shape
    owners, packed, _ = recv_ref.shape
    halves = packed // FEATS
    blocks = owners * halves
    quarters = entries // LANES
    me = lax.axis_index("cells")
    rows_pix = tiles * cells // TILE_COLS * 16
    half_width = TILE_COLS * 8.0
    wanted[...] = jnp.transpose(
        jnp.concatenate([target_ref[...], jnp.zeros((5, target_ref.shape[1]), jnp.float32)], axis=0)
    )
    row_ids = lax.broadcasted_iota(jnp.int32, (entries, entries), 0)
    col_ids = lax.broadcasted_iota(jnp.int32, (entries, entries), 1)
    before[...] = jnp.where(row_ids < col_ids, 1.0, 0.0).astype(jnp.bfloat16)
    after[...] = jnp.where(row_ids > col_ids, 1.0, 0.0).astype(jnp.bfloat16)

    def load_main(b):
        s, h = divmod(b, halves)
        return recv_ref[s, 8 * h : 8 * h + 8, :]

    def load_last(b):
        s, h = divmod(b, halves)
        return jnp.broadcast_to(recv_ref[s, 8 * halves + h : 8 * halves + h + 1, :], (8, LANES))

    slots = tiles * quarters
    for o in range(slots):
        t, q = divmod(o, quarters)
        row = lists_ref[t : t + 1, q * LANES : (q + 1) * LANES]
        order[o : o + 1, :] = row
        picks[t, 0:8, q * LANES : (q + 1) * LANES] = gather_eight(
            load_main, blocks, jnp.broadcast_to(row, (8, LANES))
        )
    for p in range(slots // 8):
        picked = gather_eight(load_last, blocks, order[8 * p : 8 * p + 8, :])
        for i in range(8):
            t, q = divmod(8 * p + i, quarters)
            picks[t, 8:9, q * LANES : (q + 1) * LANES] = picked[i : i + 1]

    def one_tile(t, carry):
        def feature(f):
            return picks[t, f : f + 1, :]

        listed = lists_ref[pl.ds(t, 1), :]
        opacity = jnp.where(listed >= 0, feature(5), 0.0)
        tile_col = 4 * lax.rem(me, TILE_COLS // 4) + lax.rem(t, 4)
        tile_row = tiles // 4 * lax.div(me, TILE_COLS // 4) + lax.div(t, 4)
        across = (lax.broadcasted_iota(jnp.int32, (16, entries), 0) + tile_col * 16).astype(jnp.float32)
        delta_col = (across + 0.5 - half_width) * (1.0 / half_width) - feature(0)
        square_term = -0.5 * feature(2) * delta_col * delta_col
        cross_term = -feature(3) * delta_col
        row_scale = -0.5 * feature(4)

        def delta_row_at(r):
            down = (jnp.full((1, entries), tile_row * 16 + r, jnp.int32)).astype(jnp.float32)
            return (down + 0.5 - rows_pix * 0.5) * (1.0 / half_width) - feature(1)

        def put_parts(r, x):
            first = x.astype(jnp.bfloat16)
            parts_s[pl.ds(r * 16, 16), :] = first
            parts_s[pl.ds(256 + r * 16, 16), :] = (x - first.astype(jnp.float32)).astype(jnp.bfloat16)

        def forward(r, carry):
            delta_row = delta_row_at(r)
            power = square_term + cross_term * delta_row + row_scale * delta_row * delta_row
            alpha = opacity * jnp.exp(power)
            alpha_s[pl.ds(r * 16, 16), :] = alpha
            put_parts(r, jnp.log(1.0 - alpha))
            return carry

        lax.fori_loop(0, 16, forward, 0, unroll=4)
        sums = jnp.dot(parts_s[...], before[...], preferred_element_type=jnp.float32)
        trans_s[...] = jnp.exp(sums[0:256] + sums[256:512])

        def errors_of(r, carry):
            weight = alpha_s[pl.ds(r * 16, 16), :] * trans_s[pl.ds(r * 16, 16), :]
            where = pl.ds(t * 256 + r * 16, 16)
            values = [jnp.sum(weight * feature(6 + k), axis=1, keepdims=True) for k in range(3)]
            lane = lax.broadcasted_iota(jnp.int32, (16, 8), 1)
            image = jnp.where(lane == 0, values[0], jnp.where(lane == 1, values[1], values[2]))
            wanted[where, :] = 2.0 * (image - wanted[where, :])
            return carry

        lax.fori_loop(0, 16, errors_of, 0, unroll=8)

        def colors_of(r, carry):
            weight = alpha_s[pl.ds(r * 16, 16), :] * trans_s[pl.ds(r * 16, 16), :]
            errors = wanted[pl.ds(t * 256 + r * 16, 16), :]
            slope = 0.0
            sums = []
            for k in range(3):
                error = errors[:, k : k + 1]
                slope = slope + error * feature(6 + k)
                sums.append(carry[k] + error * weight)
            flow = weight * slope
            flow_s[pl.ds(r * 16, 16), :] = flow
            put_parts(r, flow)
            return tuple(sums)

        empty = jnp.zeros((16, entries), jnp.float32)
        color_sums = lax.fori_loop(0, 16, colors_of, (empty, empty, empty), unroll=4)
        sums = jnp.dot(parts_s[...], after[...], preferred_element_type=jnp.float32)
        trans_s[...] = sums[0:256] + sums[256:512]

        def backward(r, carry):
            delta_row = delta_row_at(r)
            alpha = alpha_s[pl.ds(r * 16, 16), :]
            slope = flow_s[pl.ds(r * 16, 16), :] - alpha / (1.0 - alpha) * trans_s[pl.ds(r * 16, 16), :]
            return (
                carry[0] + slope,
                carry[1] + slope * delta_row,
                carry[2] + slope * (delta_row * delta_row),
            )

        plain, tilted, bent = lax.fori_loop(0, 16, backward, (empty, empty, empty), unroll=4)

        def fold(x):
            return jnp.sum(x, axis=0, keepdims=True)

        moved = plain * delta_col
        pair_s[...] = jnp.concatenate(
            [
                fold(plain),
                fold(moved),
                fold(tilted),
                fold(moved * delta_col),
                fold(tilted * delta_col),
                fold(bent),
                fold(color_sums[0]),
                fold(color_sums[1]),
                fold(color_sums[2]),
                jnp.zeros((7, entries), jnp.float32),
            ],
            axis=0,
        )
        scatter_fill(pair_s[...], listed, lhs, hot, pl.multiple_of(t * entries, entries))
        return carry

    lax.fori_loop(0, tiles, one_tile, 0)
    for b, piece in enumerate(scatter_finish(lhs, hot)):
        s, h = divmod(b, halves)
        out_ref[s, 8 * h : 8 * h + 8, :] = piece[0:8]
        out_ref[s, 8 * halves + h : 8 * halves + h + 1, :] = piece[8:9]


def owner_kernel(back_ref, plan_ref, visible_ref, cam_ref, out_ref, lhs, hot, spread):
    devices, packed, _ = back_ref.shape
    halves = packed // FEATS
    for d in range(devices):
        main = jnp.concatenate([back_ref[d, 8 * h : 8 * h + 8, :] for h in range(halves)], axis=1)
        last = jnp.concatenate(
            [back_ref[d, 8 * halves + h : 8 * halves + h + 1, :] for h in range(halves)], axis=1
        )
        g = jnp.concatenate([main, last, jnp.zeros((7, halves * LANES), jnp.float32)], axis=0)
        scatter_fill(g, plan_ref[d : d + 1, :], lhs, hot, d * halves * LANES)
    pieces = scatter_finish(lhs, hot)
    blocks = len(pieces)
    for b, piece in enumerate(pieces):
        spread[16 * b : 16 * b + 16, :] = piece
    for f in range(FEATS):
        out_ref[f] = spread[pl.ds(f, blocks, stride=16), :]
    for b in range(blocks):
        out_ref[FEATS, b : b + 1, :] = visible_ref[:, b * LANES : (b + 1) * LANES].astype(jnp.float32)
    out_ref[FEATS + 1] = jnp.broadcast_to(
        jnp.concatenate([cam_ref[...], jnp.zeros((1, LANES - 6), jnp.float32)], axis=1),
        (blocks, LANES),
    )


def update_kernel(params_ref, first_ref, second_ref, shared_ref, new_ref, new_first_ref, new_second_ref, staged, grads):
    count, block = params_ref.shape
    blocks = block // LANES
    views = shared_ref.shape[0]
    stage_rows(params_ref, staged)
    grads[...] = jnp.zeros_like(grads)

    def one_part(step, carry):
        part, view = lax.div(step, views), lax.rem(step, views)
        base = part * (8 * PAD_ROWS)
        start = pl.multiple_of(part * 8, 8)
        cam = shared_ref[view, FEATS + 1, 0:1, :]
        turn, centre = camera_terms(cam)
        rows = tuple(staged[pl.ds(base + r, 8, stride=PAD_ROWS), :] for r in range(count))
        feats, pull = jax.vjp(lambda *items: project_rows(items, turn, centre), *rows)
        got = [shared_ref[view, f, pl.ds(start, 8), :] for f in range(FEATS)]
        slopes = (
            feats[2] * got[1] + feats[3] * got[2],
            feats[3] * got[1] + feats[4] * got[2],
            -0.5 * got[3],
            -got[4],
            -0.5 * got[5],
            got[0] / feats[5],
            got[6],
            got[7],
            got[8],
        )
        for r, item in enumerate(pull(slopes)):
            where = pl.ds(base + r, 8, stride=PAD_ROWS)
            grads[where, :] = grads[where, :] + item
        return carry

    lax.fori_loop(0, blocks // 8 * views, one_part, 0)
    row_ids = lax.broadcasted_iota(jnp.int32, (count, LANES), 0)
    rates = jnp.where(
        row_ids < 6,
        0.01,
        jnp.where(
            row_ids < 10,
            0.005,
            jnp.where(row_ids < 11, 0.05, jnp.where(row_ids < 14, 0.0025, 0.000125)),
        ),
    )
    bias_one = 1.0 - 0.9**ADAM_STEP
    bias_two = 1.0 - 0.999**ADAM_STEP
    for b in range(blocks):
        span = slice(b * LANES, (b + 1) * LANES)
        gradient = grads[b * PAD_ROWS : b * PAD_ROWS + count, :]
        params, first, second = params_ref[:, span], first_ref[:, span], second_ref[:, span]
        counts = shared_ref[0, FEATS, b : b + 1, :]
        for view in range(1, views):
            counts = counts + shared_ref[view, FEATS, b : b + 1, :]
        seen = jnp.broadcast_to(counts, params.shape) > 0.0
        first_new = 0.9 * first + 0.1 * gradient
        second_new = 0.999 * second + 0.001 * gradient * gradient
        stride = rates * (first_new / bias_one) / (jnp.sqrt(second_new / bias_two) + 1e-08)
        new_ref[:, span] = jnp.where(seen, params - stride, params)
        new_first_ref[:, span] = jnp.where(seen, first_new, first)
        new_second_ref[:, span] = jnp.where(seen, second_new, second)


def fused_shards(params, first_moment, second_moment, cameras, visible, send_plan, tile_lists, target):
    cells = lax.axis_size("cells")
    count, block = params.shape
    blocks = block // LANES
    plan = send_plan[0, 0]
    lists = tile_lists[0]
    tiles, entries = lists.shape
    halves = plan.shape[1] // LANES
    slots = cells * halves
    f32, bf16 = jnp.float32, jnp.bfloat16
    packet = jax.ShapeDtypeStruct((cells, FEATS * halves, LANES), f32)
    outgoing = pl.pallas_call(
        project_kernel,
        out_shape=packet,
        scratch_shapes=[
            pltpu.VMEM((blocks * PAD_ROWS, LANES), f32),
            pltpu.VMEM((blocks * 8, LANES), f32),
            pltpu.VMEM((blocks, LANES), f32),
            pltpu.VMEM((slots, LANES), jnp.int32),
        ],
    )(params, cameras, plan)
    incoming = exchange(outgoing, "cells", True, 0)
    back = pl.pallas_call(
        functools.partial(render_kernel, cells),
        out_shape=packet,
        scratch_shapes=[
            pltpu.VMEM((tiles * entries // LANES, LANES), jnp.int32),
            pltpu.VMEM((tiles, 16, entries), f32),
            pltpu.VMEM((tiles * 256, 8), f32),
            pltpu.VMEM((entries, entries), bf16),
            pltpu.VMEM((entries, entries), bf16),
            pltpu.VMEM((256, entries), f32),
            pltpu.VMEM((256, entries), f32),
            pltpu.VMEM((256, entries), f32),
            pltpu.VMEM((512, entries), bf16),
            pltpu.VMEM((16, entries), f32),
            pltpu.VMEM((slots * 48, tiles * entries), bf16),
            pltpu.VMEM((LANES, tiles * entries), bf16),
        ],
    )(incoming, lists, target[0])
    returned = exchange(back, "cells", True, 1)
    mine = pl.pallas_call(
        owner_kernel,
        out_shape=jax.ShapeDtypeStruct((FEATS + 2, blocks, LANES), f32),
        scratch_shapes=[
            pltpu.VMEM((blocks * 48, slots * LANES), bf16),
            pltpu.VMEM((LANES, slots * LANES), bf16),
            pltpu.VMEM((blocks * 16, LANES), f32),
        ],
    )(returned, plan, visible, cameras)
    shared = exchange(mine, "views", False, 2)
    like = jax.ShapeDtypeStruct(params.shape, f32)
    return tuple(
        pl.pallas_call(
            update_kernel,
            out_shape=(like, like, like),
            scratch_shapes=[
                pltpu.VMEM((blocks * PAD_ROWS, LANES), f32),
                pltpu.VMEM((blocks * PAD_ROWS, LANES), f32),
            ],
        )(params, first_moment, second_moment, shared)
    )


def local_shards(params, first_moment, second_moment, cameras, visible, send_plan, tile_lists, target):
    capacity = send_plan.shape[3]
    tiles, entries = tile_lists.shape[1:]
    halves = capacity // LANES
    fits = (
        capacity % LANES == 0
        and params.shape[1] % (8 * LANES) == 0
        and entries % LANES == 0
        and 8 % max(halves, 1) == 0
        and lax.axis_size("cells") * halves % 8 == 0
        and tiles * entries // LANES % 8 == 0
        and tiles * entries <= 4096
        and tiles % 4 == 0
    )
    body = fused_shards if fits else shards
    return body(params, first_moment, second_moment, cameras, visible, send_plan, tile_lists, target)


def solution(mesh):
    in_specs = (
        P(None, "cells"),
        P(None, "cells"),
        P(None, "cells"),
        P("views", None),
        P("views", "cells"),
        P("views", "cells", None, None),
        P("views", "cells", None),
        P("views", None, "cells"),
    )
    out_specs = (P(None, "cells"), P(None, "cells"), P(None, "cells"))
    return jax.shard_map(local_shards, mesh=mesh, in_specs=in_specs, out_specs=out_specs, check_vma=False)
```
